32 devices in a mesh: cluster: 8 (over z, x), dir: 4 (over y, core).
Axes of the slice: x: 2, y: 2, z: 4, core: 2. Of those that a mesh axis runs over, the one named last changes fastest.
Arguments:
- ray_code: int32 [1024, 65536], P('dir', 'cluster'), may hold values from 0 to 16, as said below
- occluder_list: int32 [8, 16], replicated, may hold values from 0 to 63, as said below
- list_count: int32 [8], replicated, may hold values from 1 to 16, 96 in all
- normal_azimuth: float32 [65536], P('cluster'), may hold values from -3.140625 to 3.140625
- normal_height: float32 [65536], P('cluster'), may hold values from -1 to 1
- albedo: float32 [65536], P('cluster'), may hold values from 0.2 to 1
- occluder_exit_radiance: bfloat16 [64, 81, 1024], P('cluster', None, 'dir'), may hold values from -18 to 18
Outputs:
- transfer: bfloat16 [81, 65536], P(None, ('cluster', 'dir'))
The draws below stay inside these ranges and needn't reach their ends.
Inputs may be any that keep to these rules, and one draw needn't show every extreme that they name: `occluder_list`: each row names 16 different blocks, exactly 2 held by each of 8 different clusters; block b is held by cluster b // 8. `list_count`: entry c is the number of leading slots of row c of occluder_list in use. `ray_code`: A code of a vertex of cluster c below list_count[c] names the slot of that cluster's list whose block the ray ends on; any other code means the ray escapes.
All inputs are finite; a program needn't handle non-finite values.
Results may differ from the reference program's by a relative error of at most 0.0041.
Values may be sent and summed in bfloat16 or wider, within the bound.
No kernel may reach another device: no remote copies, remote signals or barrier semaphores. Data moves between devices by JAX's collectives and lax.ppermute only.
A program may use at most 128 MiB of HBM per device.

```python
import math
import jax
import jax.numpy as jnp
import numpy as np
from jax import lax

NDIR = 1024
SHORD = 9
LIST_SLOTS = 16
PER_OWNER = 2
BLK_DEV = 8
VERT_DEV = 8192
CLUSTERS = 8
VERTS = 65536
BLOCKS = 64
COEFFS = 81


def owner_draw(owner_key):
    return jax.random.permutation(owner_key, CLUSTERS)[:LIST_SLOTS // PER_OWNER]


def inner_draw(inner_key):
    return jax.random.permutation(inner_key, BLK_DEV)[:PER_OWNER]


def order_draw(order_key):
    return jax.random.permutation(order_key, LIST_SLOTS)


def draw_occluder_list(key, part):
    groups = LIST_SLOTS // PER_OWNER
    owner_keys = jax.random.split(jax.random.fold_in(key, 11), CLUSTERS)
    owners = jax.vmap(owner_draw)(owner_keys)
    inner_keys = jax.random.split(jax.random.fold_in(key, 12), CLUSTERS * groups)
    inner = jax.vmap(inner_draw)(inner_keys).reshape(CLUSTERS, groups, PER_OWNER)
    entries = (owners[:, :, None] * BLK_DEV + inner).reshape(CLUSTERS, LIST_SLOTS)
    order_keys = jax.random.split(jax.random.fold_in(key, 13), CLUSTERS)
    orders = jax.vmap(order_draw)(order_keys)
    return jnp.take_along_axis(entries, orders, axis=1).astype(jnp.int32)


def draw_ray_code(key, part):
    raw = jax.random.randint(jax.random.fold_in(key, 21), (NDIR, VERTS), 0, 2 * LIST_SLOTS)
    return jnp.minimum(raw, LIST_SLOTS).astype(jnp.int32)


def levels(key, dims, shards, smallest, top_value):
    def one(axis_at, blocks):
        heights = jax.random.uniform(jax.random.fold_in(jax.random.fold_in(key, 6), axis_at), (blocks,), jnp.float32, smallest / len(shards), top_value / len(shards))
        return jnp.repeat(jnp.exp(heights), dims[axis_at] // blocks).reshape((-1,) + (1,) * (len(dims) - axis_at - 1))

    gain = one(*shards[0])
    for cut in shards[1:]:
        gain = gain * one(*cut)
    return gain


def profile(count, total, reach, lean):
    portions = [(1 << 20) // math.isqrt(standing ** lean) + 1 for standing in range(2, count + 1)]
    rest, counts = total - reach - (count - 1), [1] * (count - 1)
    while rest > 0:
        free = [i for i in range(count - 1) if counts[i] < reach]
        pool, budget = sum([portions[i] for i in free]), rest
        for i in free:
            more = min(reach - counts[i], max(1, budget * portions[i] // pool), rest)
            counts[i] = counts[i] + more
            rest = rest - more
    return np.array([reach] + counts)


def ragged_sizes(stream_key, count, total, bound, slope):
    if count == 2:
        one = jax.random.randint(stream_key, (), max(1, total - bound), min(bound, total - 1) + 1)
        return jnp.stack([one, total - one])
    lengths = jnp.asarray(profile(count, total, bound, slope), jnp.int32)
    twos = (count - 1) // 2
    giver, taker = lengths[1:1 + 2 * twos:2], lengths[2:2 + 2 * twos:2]
    room = jnp.minimum(giver - 1, bound - taker)
    shifted = jax.random.randint(jax.random.fold_in(stream_key, 1), (twos,), 0, 1 << 20) % (room + 1)
    lengths = lengths.at[1:1 + 2 * twos:2].set(giver - shifted).at[2:2 + 2 * twos:2].set(taker + shifted)
    return lengths[jax.random.permutation(jax.random.fold_in(stream_key, 2), count)]


def noise(stream_key, shape, deviation, limit, cuts=(), kind=jnp.bfloat16):
    result = deviation * jax.random.normal(stream_key, shape, jnp.float32)
    if cuts:
        result = result * levels(stream_key, shape, cuts, -0.22, 0.18)
    return jnp.clip(result, -limit, limit).astype(kind)


def setup_inputs(seed: int = 0) -> dict:
    arg_keys = jax.random.split(jax.random.key(seed), 8)
    ray_code = draw_ray_code(jax.random.fold_in(arg_keys[7], 71), 0)
    occluder_list = draw_occluder_list(jax.random.fold_in(arg_keys[7], 71), 0)
    list_count = ragged_sizes(arg_keys[2], CLUSTERS, CLUSTERS * 3 * LIST_SLOTS // 4, LIST_SLOTS, 2).astype(jnp.int32)
    normal_azimuth = jnp.clip(jax.random.uniform(arg_keys[3], (VERTS,), jnp.float32, -3.140625, 3.140625), -3.140625, 3.140625)
    normal_height = jnp.clip(jax.random.uniform(arg_keys[4], (VERTS,), jnp.float32, -1.0, 1.0) * levels(arg_keys[4], (VERTS,), ((0, 8),), -0.4, 0.0), -1.0, 1.0)
    albedo = jnp.clip(jnp.exp(math.log(1.0) - 1.609438 * jax.random.uniform(arg_keys[5], (VERTS,), jnp.float32) ** levels(arg_keys[5], (VERTS,), ((0, 8),), -0.2, 0.2)), 0.2, 1.0)
    occluder_exit_radiance = noise(arg_keys[6], (BLOCKS, COEFFS, NDIR), 3.0, 18.0, ((0, 8), (2, 4)))
    return dict(ray_code=ray_code, occluder_list=occluder_list, list_count=list_count, normal_azimuth=normal_azimuth, normal_height=normal_height, albedo=albedo, occluder_exit_radiance=occluder_exit_radiance)


golden_angle = math.pi * (3.0 - math.sqrt(5.0))

def sphere_points(direction_index, direction_overall_count):
    position = direction_index.astype(jnp.float32)
    along_z = 1.0 - (2.0 * position + 1.0) / direction_overall_count
    radius = jnp.sqrt(jnp.maximum(1.0 - along_z * along_z, 0.0))
    turned = position * golden_angle
    return (radius * jnp.cos(turned), radius * jnp.sin(turned), along_z)

def harmonic_table(along_x, along_y, along_z, degrees):
    cosine_terms = [jnp.ones_like(along_x)]
    sine_terms = [jnp.zeros_like(along_x)]
    for power_exponent in range(1, degrees):
        cosine_terms.append(cosine_terms[-1] * along_x - sine_terms[-1] * along_y)
        sine_terms.append(cosine_terms[-2] * along_y + sine_terms[-1] * along_x)
    basis_rows = [None] * (degrees * degrees)
    for order_index in range(degrees):
        diagonal_entries = 1.0
        for factor in range(1, 2 * order_index, 2):
            diagonal_entries = diagonal_entries * factor
        legendre = [None] * degrees
        legendre[order_index] = jnp.full_like(along_z, diagonal_entries)
        if order_index + 1 < degrees:
            legendre[order_index + 1] = along_z * ((2 * order_index + 1) * diagonal_entries)
        for degree in range(order_index + 2, degrees):
            legendre[degree] = ((2 * degree - 1) * along_z * legendre[degree - 1] - (degree + order_index - 1) * legendre[degree - 2]) / (degree - order_index)
        for degree in range(order_index, degrees):
            factor_norm = math.sqrt((2 * degree + 1) / (4.0 * math.pi) * math.factorial(degree - order_index) / math.factorial(degree + order_index))
            centre = degree * degree + degree
            if order_index == 0:
                basis_rows[centre] = factor_norm * legendre[degree]
            else:
                basis_rows[centre + order_index] = math.sqrt(2.0) * factor_norm * legendre[degree] * cosine_terms[order_index]
                basis_rows[centre - order_index] = math.sqrt(2.0) * factor_norm * legendre[degree] * sine_terms[order_index]
    return jnp.stack(basis_rows)

def facing_table(normal_azimuth, normal_height, along_x, along_y, along_z):
    planar = jnp.sqrt(jnp.maximum(1.0 - normal_height * normal_height, 0.0))
    normal_x = planar * jnp.cos(normal_azimuth)
    normal_y = planar * jnp.sin(normal_azimuth)
    return jnp.maximum(along_x[:, None] * normal_x[None, :] + along_y[:, None] * normal_y[None, :] + along_z[:, None] * normal_height[None, :], 0.0)

def reference(ray_code, occluder_list, list_count, normal_azimuth, normal_height, albedo, occluder_exit_radiance):
    along_x, along_y, along_z = sphere_points(lax.iota(jnp.int32, NDIR), NDIR)
    harmonics = harmonic_table(along_x, along_y, along_z, SHORD)
    dir_block = min(64, NDIR)

    def per_cluster(group_cluster_index):
        first_vertex = (group_cluster_index * VERT_DEV).astype(jnp.int32)
        ray_codes = lax.dynamic_slice_in_dim(ray_code, first_vertex, VERT_DEV, 1)
        azimuths = lax.dynamic_slice_in_dim(normal_azimuth, first_vertex, VERT_DEV, 0)
        height_values = lax.dynamic_slice_in_dim(normal_height, first_vertex, VERT_DEV, 0)
        albedos = lax.dynamic_slice_in_dim(albedo, first_vertex, VERT_DEV, 0)
        facing = facing_table(azimuths, height_values, along_x, along_y, along_z)
        live_count = list_count[group_cluster_index]
        occluded = ray_codes < live_count
        direct = jnp.dot(harmonics, jnp.where(occluded, 0.0, facing), precision=lax.Precision.HIGHEST, preferred_element_type=jnp.float32)
        rounded = jnp.where(occluded, facing, 0.0).astype(jnp.bfloat16)
        weight = lax.optimization_barrier(rounded).astype(jnp.float32)
        entries = jnp.take(occluder_exit_radiance, occluder_list[group_cluster_index], axis=0).astype(jnp.float32)
        by_dir = jnp.transpose(entries, (2, 0, 1))
        safe_codes = jnp.minimum(ray_codes, LIST_SLOTS - 1)

        def add_block(block_index, total):
            first_dir = (block_index * dir_block).astype(jnp.int32)
            table = lax.dynamic_slice_in_dim(by_dir, first_dir, dir_block, 0)
            picks = lax.dynamic_slice_in_dim(safe_codes, first_dir, dir_block, 0)
            lit = lax.dynamic_slice_in_dim(weight, first_dir, dir_block, 0)
            gathered = jnp.take_along_axis(table, picks[:, :, None], axis=1)
            return total + jnp.einsum('dv,dvk->kv', lit, gathered, precision=lax.Precision.HIGHEST)
        bounce = lax.fori_loop(0, NDIR // dir_block, add_block, jnp.zeros((COEFFS, VERT_DEV), jnp.float32))
        return 4.0 * math.pi / NDIR * (direct + albedos[None, :] * bounce)
    results = lax.map(per_cluster, lax.iota(jnp.int32, CLUSTERS))
    return jnp.transpose(results, (1, 0, 2)).reshape(COEFFS, VERTS).astype(jnp.bfloat16)
```

```python
import functools
import math

import jax
import jax.numpy as jnp
import numpy as np
from jax import lax
from jax.experimental import pallas as pl
from jax.experimental.pallas import tpu as pltpu
from jax.sharding import PartitionSpec as P

NDIR = 1024
SHORD = 9
PER_OWNER = 2
TILE = 256
ESCAPED = 255


golden_angle = math.pi * (3.0 - math.sqrt(5.0))


def sphere_points(count):
    position = np.arange(count, dtype=np.float32)
    along_z = np.float32(1.0) - (np.float32(2.0) * position + np.float32(1.0)) / np.float32(count)
    radius = np.sqrt(np.maximum(np.float32(1.0) - along_z * along_z, np.float32(0.0)))
    turned = position * np.float32(golden_angle)
    return radius * np.cos(turned), radius * np.sin(turned), along_z


def harmonic_table(along_x, along_y, along_z, degrees):
    x, y, z = (a.astype(np.float64) for a in (along_x, along_y, along_z))
    cosine, sine = [np.ones_like(x)], [np.zeros_like(x)]
    for _ in range(1, degrees):
        cosine.append(cosine[-1] * x - sine[-1] * y)
        sine.append(cosine[-2] * y + sine[-1] * x)
    rows = [None] * (degrees * degrees)
    for order in range(degrees):
        diagonal = 1.0
        for factor in range(1, 2 * order, 2):
            diagonal = diagonal * factor
        legendre = [None] * degrees
        legendre[order] = np.full_like(z, diagonal)
        if order + 1 < degrees:
            legendre[order + 1] = z * ((2 * order + 1) * diagonal)
        for degree in range(order + 2, degrees):
            legendre[degree] = (
                (2 * degree - 1) * z * legendre[degree - 1] - (degree + order - 1) * legendre[degree - 2]
            ) / (degree - order)
        for degree in range(order, degrees):
            norm = math.sqrt(
                (2 * degree + 1) / (4.0 * math.pi) * math.factorial(degree - order) / math.factorial(degree + order)
            )
            centre = degree * degree + degree
            if order == 0:
                rows[centre] = norm * legendre[degree]
            else:
                rows[centre + order] = math.sqrt(2.0) * norm * legendre[degree] * cosine[order]
                rows[centre - order] = math.sqrt(2.0) * norm * legendre[degree] * sine[order]
    return np.stack(rows)


def padded(rows):
    return -(-rows // 16) * 16


def smem():
    return pl.BlockSpec(memory_space=pltpu.SMEM)


def vmem():
    return pl.BlockSpec(memory_space=pltpu.VMEM)


def limits(mebibytes):
    return pltpu.CompilerParams(dimension_semantics=("arbitrary",), vmem_limit_bytes=mebibytes << 20)


def outgoing_kernel(clusters, slots, held, coeffs, me_ref, list_ref, blocks_ref, slot_ref, *refs):
    out_refs, (wide_ref, pair_ref) = refs[:clusters], refs[clusters:]
    me = me_ref[0]
    dirs = blocks_ref.shape[-1]
    for h in range(2):
        wide_ref[h] = blocks_ref[:, :, h * 128 : h * 128 + 128].astype(jnp.float32).reshape(coeffs * held, dirs // 2)

    def pick(row, owner, base):
        low, high = owner * held, owner * held + held
        found = [jnp.int32(-1)] * PER_OWNER
        seen = jnp.int32(0)
        for s in range(slots):
            entry = list_ref[row, s]
            mine = (entry >= low) & (entry < high)
            value = (entry - low) if base else jnp.int32(s)
            for p in range(PER_OWNER):
                found[p] = jnp.where(mine & (seen == p), value, found[p])
            seen = seen + mine.astype(jnp.int32)
        return found

    for k in reversed(range(clusters)):
        other = jnp.bitwise_xor(me, k)
        blocks = pick(other, me, True)
        for p in range(PER_OWNER):
            row = jnp.maximum(blocks[p], 0)
            for h in range(2):
                pair_ref[h, pl.ds(coeffs * p, coeffs), :] = wide_ref[h, pl.ds(row, coeffs, held), :]
        for h in range(2):
            out_refs[k][:, h * 128 : h * 128 + 128] = pair_ref[h].astype(jnp.bfloat16)
        mine = pick(me, other, False)
        for p in range(PER_OWNER):
            slot_ref[PER_OWNER * k + p] = mine[p]


def outgoing_pairs(me, occluder_list, blocks):
    clusters, slots = occluder_list.shape
    coeffs, held, dirs = blocks.shape
    pair = jax.ShapeDtypeStruct((PER_OWNER * coeffs, dirs), blocks.dtype)
    result = pl.pallas_call(
        functools.partial(outgoing_kernel, clusters, slots, held, coeffs),
        out_shape=[jax.ShapeDtypeStruct((PER_OWNER * clusters,), jnp.int32)] + [pair] * clusters,
        in_specs=[smem(), smem(), vmem()],
        out_specs=[smem()] + [vmem()] * clusters,
        scratch_shapes=[
            pltpu.VMEM((2, coeffs * held, dirs // 2), jnp.float32),
            pltpu.VMEM((2, PER_OWNER * coeffs, dirs // 2), jnp.float32),
        ],
        compiler_params=pltpu.CompilerParams(vmem_limit_bytes=8 << 20),
        name="outgoing",
    )(me, occluder_list, blocks)
    return result[0], result[1:]


def accumulators(coeffs_padded, count):
    return [pltpu.ACC(q)((coeffs_padded, TILE), jnp.float32) for _ in range(count) for q in (0, 1)]


def bounce_passes(code, weight, lhs_ref, slot_ref, first, pairs, accs, stage):
    zero = jnp.zeros((), jnp.bfloat16)
    for i in range(pairs):
        for q in (0, 1):
            slot = slot_ref[first + PER_OWNER * i + q].astype(jnp.float32).astype(jnp.bfloat16)
            spread = jnp.where(code == slot, weight, zero)
            pltpu.matmul_push_rhs(spread, staging_register=stage % 2, mxu_index=q)
            pltpu.matmul_acc_lhs(accs[q], joined(lhs_ref, PER_OWNER * i + q), load_staged_rhs=stage % 2)
        stage += 1
    return stage


def joined(ref, index):
    return jnp.concatenate([ref[index, 0], ref[index, 1]], axis=1)


def fill_lhs(lhs_ref, wide_ref, pair_refs, coeffs):
    wide_ref[...] = jnp.zeros_like(wide_ref)
    for i, ref in enumerate(pair_refs):
        wide_ref[i % 2, : ref.shape[0], :] = ref[...].astype(jnp.float32)
        for p in range(PER_OWNER):
            block = wide_ref[i % 2, pl.ds(coeffs * p, lhs_ref.shape[2]), :].astype(jnp.bfloat16)
            lhs_ref[PER_OWNER * i + p, 0] = block[:, :128]
            lhs_ref[PER_OWNER * i + p, 1] = block[:, 128:]


def near_kernel(
    pairs, coeffs, first, chunk,
    part_ref, me_ref, count_ref, slot_ref, code_ref, nx_ref, ny_ref, nz_ref, albedo_ref,
    dirs_ref, high_ref, low_ref, *rest,
):
    pair_refs, (total_ref, code_out, weight_out, axis_ref, lhs_ref, wide_ref) = rest[:pairs], rest[pairs:]
    rows = code_ref.shape[0]
    step = pl.program_id(0)

    @pl.when(step == 0)
    def _():
        for a in range(3):
            axis_ref[a] = jnp.broadcast_to(dirs_ref[:, a : a + 1], (rows, 128))
        if pairs:
            fill_lhs(lhs_ref, wide_ref, pair_refs, coeffs)

    live = count_ref[me_ref[0]]
    height = padded(coeffs)

    def body(*accs):
        stage = 0
        for t in range(chunk):
            at = step * chunk + t
            for h in range(2):
                cols = pl.ds(pl.multiple_of(at * TILE + h * 128, 128), 128)
                facing = jnp.maximum(
                    axis_ref[0] * nx_ref[:, cols] + axis_ref[1] * ny_ref[:, cols] + axis_ref[2] * nz_ref[:, cols],
                    0.0,
                )
                raw = code_ref[:, t * TILE + h * 128 : t * TILE + h * 128 + 128]
                known = jnp.where(raw < live, raw, ESCAPED)
                code_out[at, h] = known.astype(jnp.float32).astype(jnp.bfloat16)
                weight_out[at, h] = facing.astype(jnp.bfloat16)
            code = joined(code_out, at)
            weight = joined(weight_out, at)
            use = accs[4 * (t % 2) : 4 * (t % 2) + 4]
            lit = jnp.where(code == jnp.bfloat16(ESCAPED), weight, jnp.zeros((), jnp.bfloat16))
            for q, table in ((0, high_ref), (1, low_ref)):
                pltpu.matmul_push_rhs(lit, staging_register=stage % 2, mxu_index=q)
                pltpu.matmul_acc_lhs(use[q], table[...], load_staged_rhs=stage % 2)
            stage += 1
            if pairs:
                stage = bounce_passes(code, weight, lhs_ref, slot_ref, first, pairs, use[2:], stage)
            direct = pltpu.matmul_pop(use[0]) + pltpu.matmul_pop(use[1])
            if pairs:
                bounce = pltpu.matmul_pop(use[2]) + pltpu.matmul_pop(use[3])
                direct = direct + albedo_ref[:, pl.ds(pl.multiple_of(at * TILE, TILE), TILE)] * bounce
            total_ref[at] = direct[:coeffs]

    pl.run_scoped(body, *accumulators(height, 4))


def near_pass(part, me, count, slots, codes, normals, albedo, dirs, high, low, pairs, first, chunk):
    rows, verts = codes.shape
    coeffs = SHORD * SHORD
    height = padded(coeffs)
    tiles = verts // TILE
    grid_spec = pltpu.PrefetchScalarGridSpec(
        num_scalar_prefetch=1,
        grid=(tiles // chunk,),
        in_specs=[smem(), smem(), smem(), pl.BlockSpec((rows, chunk * TILE), lambda i, p: (0, i))]
        + [vmem()] * 4
        + [
            pl.BlockSpec((rows, 4), lambda i, p: (p[0], 0)),
            pl.BlockSpec((height, rows), lambda i, p: (0, p[0])),
            pl.BlockSpec((height, rows), lambda i, p: (0, p[0])),
        ]
        + [vmem()] * len(pairs),
        out_specs=[vmem()] * 3,
        scratch_shapes=[
            pltpu.VMEM((3, rows, 128), jnp.float32),
            pltpu.VMEM((max(1, len(pairs)) * PER_OWNER, 2, height, rows // 2), jnp.bfloat16),
            pltpu.VMEM((2, coeffs + height + 8, rows), jnp.float32),
        ],
    )
    flops = 2 * height * rows * verts * (2 + 2 * len(pairs))
    return pl.pallas_call(
        functools.partial(near_kernel, len(pairs), coeffs, first, chunk),
        grid_spec=grid_spec,
        out_shape=[
            jax.ShapeDtypeStruct((tiles, coeffs, TILE), jnp.float32),
            jax.ShapeDtypeStruct((tiles, 2, rows, TILE // 2), jnp.bfloat16),
            jax.ShapeDtypeStruct((tiles, 2, rows, TILE // 2), jnp.bfloat16),
        ],
        compiler_params=limits(40),
        cost_estimate=pl.CostEstimate(flops=flops, bytes_accessed=20 << 20, transcendentals=0),
        name="near",
    )(part, me, count, slots, codes, *normals, albedo, dirs, high, low, *pairs)


def far_kernel(pairs, coeffs, first, unpack, added, scale, shift, chunk, part_ref, slot_ref, code_ref, weight_ref, total_ref, albedo_ref, *rest):
    if unpack:
        pair_refs, rest = rest[:pairs], rest[pairs:]
    else:
        lhs_ref, rest = rest[0], rest[1:]
    if added:
        add_ref, rest = rest[0], rest[1:]
    out_ref, rest = rest[0], rest[1:]
    step = pl.program_id(0)
    if unpack:
        lhs_ref, wide_ref = rest

        @pl.when(step == 0)
        def _():
            fill_lhs(lhs_ref, wide_ref, pair_refs, coeffs)

    base = jnp.bitwise_xor(part_ref[0], shift) * (pl.num_programs(0) * chunk) + step * chunk

    def body(*accs):
        stage = 0
        for t in range(chunk):
            at = base + t
            use = accs[2 * (t % 4) : 2 * (t % 4) + 2]
            code, weight = joined(code_ref, at), joined(weight_ref, at)
            stage = bounce_passes(code, weight, lhs_ref, slot_ref, first, pairs, use, stage)
            bounce = pltpu.matmul_pop(use[0]) + pltpu.matmul_pop(use[1])
            light = albedo_ref[:, pl.ds(pl.multiple_of(at * TILE, TILE), TILE)]
            result = scale * (total_ref[at] + light * bounce[:coeffs])
            tile = slice(t * TILE, t * TILE + TILE)
            if added:
                result = result + add_ref[:, pl.ds(pl.multiple_of((step * chunk + t) * TILE, TILE), TILE)].astype(jnp.float32)
            out_ref[:, tile] = result.astype(out_ref.dtype)

    pl.run_scoped(body, *accumulators(padded(coeffs), 4))


def far_pass(part, slots, codes, weights, total, albedo, source, first, count, shift, added, dtype, shards, chunk):
    tiles, coeffs, _ = total.shape
    rows = codes.shape[2]
    height = padded(coeffs)
    share = tiles // shards
    unpack = isinstance(source, list)
    operands = list(source) if unpack else [source]
    lhs_shape = (count * PER_OWNER, 2, height, rows // 2)
    extra = [jax.ShapeDtypeStruct(lhs_shape, jnp.bfloat16)] if unpack else []
    grid_spec = pltpu.PrefetchScalarGridSpec(
        num_scalar_prefetch=1,
        grid=(share // chunk,),
        in_specs=[smem()] + [vmem()] * (4 + len(operands) + (added is not None)),
        out_specs=[pl.BlockSpec((coeffs, chunk * TILE), lambda i, p: (0, i))] + [vmem()] * len(extra),
        scratch_shapes=[pltpu.VMEM((2, coeffs + height + 8, rows), jnp.float32)] * unpack,
    )
    flops = 2 * height * rows * share * TILE * 2 * count
    result = pl.pallas_call(
        functools.partial(
            far_kernel, count, coeffs, first, unpack, added is not None, 4.0 * math.pi / NDIR, shift, chunk
        ),
        grid_spec=grid_spec,
        out_shape=[jax.ShapeDtypeStruct((coeffs, share * TILE), dtype)] + extra,
        compiler_params=limits(24),
        cost_estimate=pl.CostEstimate(flops=flops, bytes_accessed=4 << 20, transcendentals=0),
        name=f"far_{shift}",
    )(part, slots, codes, weights, total, albedo, *operands, *([] if added is None else [added]))
    return (result[0], result[1]) if unpack else result[0]


def listed_by_exchange(me, occluder_list, blocks):
    clusters, slots = occluder_list.shape
    held, coeffs, dirs = blocks.shape
    slot_index = lax.iota(jnp.int32, slots)
    owners = occluder_list // held
    here = owners == me
    position = jnp.cumsum(here.astype(jnp.int32), axis=1) - 1
    matched = here[:, None, :] & (position[:, None, :] == lax.iota(jnp.int32, PER_OWNER)[None, :, None])
    chosen = jnp.sum(jnp.where(matched, (occluder_list - me * held)[:, None, :], 0), axis=2)
    outgoing = jnp.take(blocks, chosen, axis=0)
    incoming = lax.all_to_all(outgoing, "cluster", split_axis=0, concat_axis=0, tiled=True)
    own = owners[me]
    earlier = (own[None, :] == own[:, None]) & (slot_index[None, :] < slot_index[:, None])
    row = own * PER_OWNER + jnp.sum(earlier.astype(jnp.int32), axis=1)
    entries = jnp.take(incoming.reshape(clusters * PER_OWNER, coeffs, dirs), row, axis=0)
    pairs = entries.reshape(slots // PER_OWNER, PER_OWNER * coeffs, dirs)
    return slot_index, [pairs[i] for i in range(slots // PER_OWNER)]


def per_device(n_cluster, n_dir, ray_code, occluder_list, list_count, normal_azimuth, normal_height, albedo, radiance):
    rows, verts = ray_code.shape
    me = lax.axis_index("cluster").astype(jnp.int32)
    part = lax.axis_index("dir").astype(jnp.int32)[None]

    axis_x, axis_y, axis_z = sphere_points(NDIR)
    table = harmonic_table(axis_x, axis_y, axis_z, SHORD).astype(np.float32)
    table = np.pad(table, ((0, padded(table.shape[0]) - table.shape[0]), (0, 0)))
    high = table.astype(jnp.bfloat16)
    low = (table - high.astype(np.float32)).astype(jnp.bfloat16)
    dirs = np.stack([axis_x, axis_y, axis_z, np.zeros_like(axis_x)], axis=1)

    if n_cluster <= 8 and n_cluster & (n_cluster - 1) == 0:
        slots, outgoing = outgoing_pairs(me[None], occluder_list, jnp.transpose(radiance, (1, 0, 2)))
        pairs = list(outgoing)
        for k in reversed(range(1, n_cluster)):
            pairs[k] = lax.ppermute(outgoing[k], "cluster", [(i, i ^ k) for i in range(n_cluster)])
    else:
        slots, pairs = listed_by_exchange(me, occluder_list, radiance)
    split = len(pairs) // 2

    planar = jnp.sqrt(jnp.maximum(1.0 - normal_height * normal_height, 0.0))
    normals = [planar * jnp.cos(normal_azimuth), planar * jnp.sin(normal_azimuth), normal_height]
    normals = [n[None, :] for n in normals]
    albedo = albedo[None, :]

    chunk = min(4, verts // n_dir // TILE)
    total, codes, weights = near_pass(
        part, me[None], list_count, slots, ray_code, normals, albedo, jnp.asarray(dirs), jnp.asarray(high), jnp.asarray(low),
        pairs[:split], 0, chunk,
    )

    def far(source, shift, added, dtype):
        return far_pass(
            part, slots, codes, weights, total, albedo, source, PER_OWNER * split, len(pairs) - split, shift, added, dtype,
            n_dir, chunk,
        )

    def swap(value, mask):
        return lax.ppermute(value, "dir", [(i, i ^ mask) for i in range(n_dir)])

    if n_dir == 4:
        part_3, lhs = far(pairs[split:], 3, None, jnp.bfloat16)
        part_2 = swap(far(lhs, 2, swap(part_3, 1), jnp.bfloat16), 2)
        part_1 = swap(far(lhs, 1, None, jnp.bfloat16), 1)
        kept = far(lhs, 0, part_1, jnp.float32)
        return (kept + part_2.astype(jnp.float32)).astype(jnp.bfloat16)
    kept, lhs = far(pairs[split:], 0, None, jnp.float32)
    for mask in range(1, n_dir):
        kept = kept + swap(far(lhs, mask, None, jnp.bfloat16), mask).astype(jnp.float32)
    return kept.astype(jnp.bfloat16)


def solution(mesh):
    return jax.shard_map(
        functools.partial(per_device, mesh.shape["cluster"], mesh.shape["dir"]),
        mesh=mesh,
        in_specs=(P("dir", "cluster"), P(), P(), P("cluster"), P("cluster"), P("cluster"), P("cluster", None, "dir")),
        out_specs=P(None, ("cluster", "dir")),
        check_vma=False,
    )
```

```python
import functools
import math

import jax
import jax.numpy as jnp
import numpy as np
from jax import lax
from jax.experimental import pallas as pl
from jax.experimental.pallas import tpu as pltpu
from jax.sharding import PartitionSpec as P

NDIR = 1024
SHORD = 9
PER_OWNER = 2
TILE = 256
ESCAPED = 255
STRIPS = 4


golden_angle = math.pi * (3.0 - math.sqrt(5.0))


def sphere_points(count):
    position = np.arange(count, dtype=np.float32)
    along_z = np.float32(1.0) - (np.float32(2.0) * position + np.float32(1.0)) / np.float32(count)
    radius = np.sqrt(np.maximum(np.float32(1.0) - along_z * along_z, np.float32(0.0)))
    turned = position * np.float32(golden_angle)
    return radius * np.cos(turned), radius * np.sin(turned), along_z


def harmonic_table(along_x, along_y, along_z, degrees):
    x, y, z = (a.astype(np.float64) for a in (along_x, along_y, along_z))
    cosine, sine = [np.ones_like(x)], [np.zeros_like(x)]
    for _ in range(1, degrees):
        cosine.append(cosine[-1] * x - sine[-1] * y)
        sine.append(cosine[-2] * y + sine[-1] * x)
    rows = [None] * (degrees * degrees)
    for order in range(degrees):
        diagonal = 1.0
        for factor in range(1, 2 * order, 2):
            diagonal = diagonal * factor
        legendre = [None] * degrees
        legendre[order] = np.full_like(z, diagonal)
        if order + 1 < degrees:
            legendre[order + 1] = z * ((2 * order + 1) * diagonal)
        for degree in range(order + 2, degrees):
            legendre[degree] = (
                (2 * degree - 1) * z * legendre[degree - 1] - (degree + order - 1) * legendre[degree - 2]
            ) / (degree - order)
        for degree in range(order, degrees):
            norm = math.sqrt(
                (2 * degree + 1) / (4.0 * math.pi) * math.factorial(degree - order) / math.factorial(degree + order)
            )
            centre = degree * degree + degree
            if order == 0:
                rows[centre] = norm * legendre[degree]
            else:
                rows[centre + order] = math.sqrt(2.0) * norm * legendre[degree] * cosine[order]
                rows[centre - order] = math.sqrt(2.0) * norm * legendre[degree] * sine[order]
    return np.stack(rows)


def padded(rows):
    return -(-rows // 16) * 16


def smem():
    return pl.BlockSpec(memory_space=pltpu.SMEM)


def hbm():
    return pl.BlockSpec(memory_space=pltpu.HBM)


def pinned(value):
    return pltpu.with_memory_space_constraint(value, pltpu.HBM)


def vmem():
    return pl.BlockSpec(memory_space=pltpu.VMEM)


def limits(mebibytes):
    return pltpu.CompilerParams(dimension_semantics=("arbitrary",), vmem_limit_bytes=mebibytes << 20)


def outgoing_kernel(clusters, slots, held, coeffs, *refs):
    list_hbm, count_hbm, blocks_hbm = refs[:3]
    table_hbms, refs = refs[3:9], refs[9:]
    slot_ref, live_ref = refs[:2]
    table_refs, refs = refs[2:7], refs[7:]
    out_refs = refs[clusters - 1 :: -1] if clusters else ()
    list_ref, count_ref, blocks_ref, wide_ref, pair_ref, sems, table_sems = refs[clusters:]
    loads = table_copies(table_hbms, table_refs, table_sems)
    half = blocks_ref.shape[-1] // 2
    copies = [
        pltpu.make_async_copy(source, target, sems.at[i])
        for i, (source, target) in enumerate(
            [(list_hbm, list_ref), (count_hbm, count_ref), (blocks_hbm, blocks_ref)]
        )
    ]
    for copy in copies + loads:
        copy.start()
    me = lax.axis_index("cluster").astype(jnp.int32)
    copies[0].wait()
    copies[1].wait()
    live_ref[...] = jnp.full(live_ref.shape, count_ref[me].astype(jnp.float32), jnp.float32).astype(jnp.bfloat16)

    def pick(row, owner, base):
        first, last = jnp.int32(0 if base else -1), jnp.int32(0 if base else -1)
        entries = [list_ref[row, s] - owner * held for s in range(slots)]
        mine = [(e >= 0) & (e < held) for e in entries]
        for s in range(slots):
            last = jnp.where(mine[s], entries[s] if base else s, last)
        for s in reversed(range(slots)):
            first = jnp.where(mine[s], entries[s] if base else s, first)
        return first, last

    chosen = [pick(jnp.bitwise_xor(me, k), me, True) for k in range(clusters)]
    copies[2].wait()
    for h in range(2):
        part = blocks_ref[:, :, h * half : h * half + half]
        wide_ref[h] = part.astype(jnp.float32).reshape(coeffs * held, half)
    for k in range(clusters):
        for p in range(PER_OWNER):
            for h in range(2):
                pair_ref[h, pl.ds(coeffs * p, coeffs), :] = wide_ref[h, pl.ds(chosen[k][p], coeffs, held), :]
        for h in range(2):
            out_refs[k][:, h * half : h * half + half] = pair_ref[h].astype(jnp.bfloat16)
    for k in range(clusters):
        slots_k = pick(me, jnp.bitwise_xor(me, k), False)
        for p in range(PER_OWNER):
            value = jnp.full(slot_ref.shape[1:], slots_k[p].astype(jnp.float32), jnp.float32)
            slot_ref[PER_OWNER * k + p] = value.astype(jnp.bfloat16)
    for copy in loads:
        copy.wait()


def table_copies(sources, targets, sems):
    azimuth, height, albedo, dirs, high, low = sources
    dirs_ref, table_ref = targets[3:]
    rows = dirs_ref.shape[0]
    part = lax.axis_index("dir").astype(jnp.int32)
    moves = [
        (azimuth, targets[0]),
        (height, targets[1]),
        (albedo, targets[2]),
        (dirs.at[pl.ds(pl.multiple_of(part * rows, rows), rows), :], dirs_ref),
    ]
    for h in range(2):
        mine = pl.ds(pl.multiple_of(part * rows + h * 128, 128), 128)
        moves.append((high.at[:, mine], table_ref.at[0, h]))
        moves.append((low.at[:, mine], table_ref.at[1, h]))
    return [pltpu.make_async_copy(*move, sems.at[i]) for i, move in enumerate(moves)]


def table_shapes(sources, rows):
    azimuth, height, albedo, dirs, high, low = sources
    shapes = [jax.ShapeDtypeStruct(a.shape, a.dtype) for a in (azimuth, height, albedo)]
    shapes.append(jax.ShapeDtypeStruct((rows, dirs.shape[1]), dirs.dtype))
    return shapes + [jax.ShapeDtypeStruct((2, 2, high.shape[0], rows // 2), high.dtype)]


def tables_kernel(*refs):
    loads = table_copies(refs[:6], refs[6:11], refs[11])
    for copy in loads:
        copy.start()
    for copy in loads:
        copy.wait()


def loaded_tables(sources, rows):
    return pl.pallas_call(
        tables_kernel,
        out_shape=table_shapes(sources, rows),
        in_specs=[hbm()] * 6,
        out_specs=[vmem()] * 5,
        scratch_shapes=[pltpu.SemaphoreType.DMA((8,))],
        compiler_params=pltpu.CompilerParams(vmem_limit_bytes=8 << 20),
        name="tables",
    )(*(pinned(a) for a in sources))


def outgoing_pairs(occluder_list, list_count, blocks, tables):
    clusters, slots = occluder_list.shape
    coeffs, held, dirs = blocks.shape
    pair = jax.ShapeDtypeStruct((PER_OWNER * coeffs, dirs), blocks.dtype)
    result = pl.pallas_call(
        functools.partial(outgoing_kernel, clusters, slots, held, coeffs),
        out_shape=[
            jax.ShapeDtypeStruct((PER_OWNER * clusters, 16, 128), jnp.bfloat16),
            jax.ShapeDtypeStruct((16, 128), jnp.bfloat16),
        ]
        + table_shapes(tables, dirs)
        + [pair] * clusters,
        in_specs=[hbm()] * 9,
        out_specs=[vmem()] * (7 + clusters),
        scratch_shapes=[
            pltpu.SMEM(occluder_list.shape, jnp.int32),
            pltpu.SMEM(list_count.shape, jnp.int32),
            pltpu.VMEM(blocks.shape, blocks.dtype),
            pltpu.VMEM((2, coeffs * held, dirs // 2), jnp.float32),
            pltpu.VMEM((2, PER_OWNER * coeffs, dirs // 2), jnp.float32),
            pltpu.SemaphoreType.DMA((3,)),
            pltpu.SemaphoreType.DMA((8,)),
        ],
        compiler_params=pltpu.CompilerParams(vmem_limit_bytes=8 << 20),
        name="outgoing",
    )(*(pinned(a) for a in (occluder_list, list_count, blocks, *tables)))
    return result[0], result[1], result[2:7], result[:6:-1]


def accumulators(coeffs_padded, count):
    return [pltpu.ACC(q)((coeffs_padded, TILE), jnp.float32) for _ in range(count) for q in (0, 1)]


def bounce_passes(code, weight, lhs_ref, slot_ref, first, pairs, accs, stage, base=0):
    zero = jnp.zeros((), jnp.bfloat16)
    for i in range(pairs):
        for q in (0, 1):
            slot = slot_ref[first + PER_OWNER * i + q]
            slot = jnp.concatenate([slot] * (code.shape[1] // 128), axis=1)
            slot = jnp.concatenate([slot] * (code.shape[0] // 16), axis=0)
            spread = jnp.where(code == slot, weight, zero)
            pltpu.matmul_push_rhs(spread, staging_register=stage % 2, mxu_index=q)
            pltpu.matmul_acc_lhs(accs[q], joined(lhs_ref, PER_OWNER * (base + i) + q), load_staged_rhs=stage % 2)
        stage += 1
    return stage


def joined(ref, index, first=0):
    return jnp.concatenate([ref[index, first], ref[index, first + 1]], axis=1)


def fill_lhs(lhs_ref, wide_ref, pair_refs, coeffs):
    wide_ref[...] = jnp.zeros_like(wide_ref)
    for i, ref in enumerate(pair_refs):
        wide_ref[i % 2, : ref.shape[0], :] = ref[...].astype(jnp.float32)
        for p in range(PER_OWNER):
            block = wide_ref[i % 2, pl.ds(coeffs * p, lhs_ref.shape[2]), :].astype(jnp.bfloat16)
            lhs_ref[PER_OWNER * i + p, 0] = block[:, :128]
            lhs_ref[PER_OWNER * i + p, 1] = block[:, 128:]


def near_kernel(
    pairs, coeffs, first, chunk,
    slot_ref, live_ref, code_ref, azimuth_ref, height_ref, albedo_ref, dirs_ref, table_ref, *rest,
):
    pair_refs, rest = rest[:pairs], rest[pairs:]
    total_ref, both_ref = rest[:2]
    normal_ref, axis_ref, lhs_ref, wide_ref = rest[2:]
    rows = code_ref.shape[0]
    step = pl.program_id(0)

    @pl.when(step == 0)
    def _():
        if pairs:
            fill_lhs(lhs_ref, wide_ref, pair_refs, coeffs)
        azimuth, height = azimuth_ref[...], height_ref[...]
        planar = jnp.sqrt(jnp.maximum(1.0 - height * height, 0.0))
        normal_ref[0] = planar * jnp.cos(azimuth)
        normal_ref[1] = planar * jnp.sin(azimuth)
        normal_ref[2] = height
        for a in range(3):
            axis_ref[a] = jnp.broadcast_to(dirs_ref[:, a : a + 1], (rows, 128))

    zero = jnp.zeros((), jnp.bfloat16)
    strip = rows // STRIPS
    live = jnp.concatenate([live_ref[...]] * (strip // 16), axis=0)

    def prepare(t, r):
        at = step * chunk + t
        band = slice(r * strip, r * strip + strip)
        along = [axis_ref[a, band] for a in range(3)]
        for h in range(2):
            line = pl.ds(at * 2 + h, 1)
            facing = along[0] * normal_ref[0, line, :] + along[1] * normal_ref[1, line, :]
            facing = facing + along[2] * normal_ref[2, line, :]
            both_ref[at, 2 + h, band] = jnp.maximum(facing.astype(jnp.bfloat16), zero)
            raw = code_ref[band, t * TILE + h * 128 : t * TILE + h * 128 + 128]
            raw = raw.astype(jnp.float32).astype(jnp.bfloat16)
            both_ref[at, h, band] = jnp.where(raw < live, raw, jnp.bfloat16(ESCAPED))

    def body(*accs):
        def finish(t):
            at = step * chunk + t
            use = accs[4 * (t % 2) : 4 * (t % 2) + 4]
            direct = pltpu.matmul_pop(use[0]) + pltpu.matmul_pop(use[1])
            if pairs:
                bounce = pltpu.matmul_pop(use[2]) + pltpu.matmul_pop(use[3])
                direct = direct + row_pair(albedo_ref, at) * bounce
            total_ref[at] = direct[:coeffs]

        for r in range(STRIPS):
            prepare(0, r)
        stage = 0
        for t in range(chunk):
            at = step * chunk + t
            code, weight = joined(both_ref, at), joined(both_ref, at, 2)
            use = accs[4 * (t % 2) : 4 * (t % 2) + 4]
            lit = jnp.where(code == jnp.bfloat16(ESCAPED), weight, zero)
            for q in (0, 1):
                pltpu.matmul_push_rhs(lit, staging_register=stage % 2, mxu_index=q)
                pltpu.matmul_acc_lhs(use[q], joined(table_ref, q), load_staged_rhs=stage % 2)
            stage += 1
            if t:
                finish(t - 1)
            todo = list(range(STRIPS)) if t + 1 < chunk else []
            for i in range(pairs):
                if todo:
                    prepare(t + 1, todo.pop(0))
                stage = bounce_passes(code, weight, lhs_ref, slot_ref, first + PER_OWNER * i, 1, use[2:], stage, i)
            for r in todo:
                prepare(t + 1, r)
        finish(chunk - 1)

    pl.run_scoped(body, *accumulators(padded(coeffs), 4))


def row_pair(ref, index):
    return jnp.concatenate([ref[pl.ds(index * 2, 1), :], ref[pl.ds(index * 2 + 1, 1), :]], axis=1)


def near_pass(slots, live, codes, tables, pairs, first, chunk):
    rows, verts = codes.shape
    coeffs = SHORD * SHORD
    tall = padded(coeffs)
    tiles = verts // TILE
    flops = 2 * tall * rows * verts * (2 + 2 * len(pairs))
    return pl.pallas_call(
        functools.partial(near_kernel, len(pairs), coeffs, first, chunk),
        grid=(tiles // chunk,),
        in_specs=[vmem(), vmem(), pl.BlockSpec((rows, chunk * TILE), lambda i: (0, i))]
        + [vmem()] * (5 + len(pairs)),
        out_specs=[vmem()] * 2,
        out_shape=[
            jax.ShapeDtypeStruct((tiles, coeffs, TILE), jnp.float32),
            jax.ShapeDtypeStruct((tiles, 4, rows, TILE // 2), jnp.bfloat16),
        ],
        scratch_shapes=[
            pltpu.VMEM((3, verts // 128, 128), jnp.float32),
            pltpu.VMEM((3, rows, 128), jnp.float32),
            pltpu.VMEM((max(1, len(pairs)) * PER_OWNER, 2, tall, rows // 2), jnp.bfloat16),
            pltpu.VMEM((2, coeffs + tall + 8, rows), jnp.float32),
        ],
        compiler_params=limits(24),
        cost_estimate=pl.CostEstimate(flops=flops, bytes_accessed=20 << 20, transcendentals=0),
        name="near",
    )(slots, live, pinned(codes), *tables, *pairs)


def far_kernel(pairs, coeffs, first, unpack, added, scale, shift, chunk, slot_ref, both_ref, total_ref, albedo_ref, *rest):
    if unpack:
        pair_refs, rest = rest[:pairs], rest[pairs:]
    else:
        lhs_ref, rest = rest[0], rest[1:]
    if added:
        add_ref, rest = rest[0], rest[1:]
    out_ref, rest = rest[0], rest[1:]
    step = pl.program_id(0)
    if unpack:
        lhs_ref, wide_ref = rest

        @pl.when(step == 0)
        def _():
            fill_lhs(lhs_ref, wide_ref, pair_refs, coeffs)

    part = lax.axis_index("dir").astype(jnp.int32)
    base = jnp.bitwise_xor(part, shift) * (out_ref.shape[1] // TILE) + step * chunk

    def body(*accs):
        def finish(t):
            at = base + t
            use = accs[2 * (t % 4) : 2 * (t % 4) + 2]
            bounce = pltpu.matmul_pop(use[0]) + pltpu.matmul_pop(use[1])
            result = scale * (total_ref[at] + row_pair(albedo_ref, at) * bounce[:coeffs])
            tile = pl.ds(pl.multiple_of((step * chunk + t) * TILE, TILE), TILE)
            if added:
                result = result + add_ref[:, tile].astype(jnp.float32)
            out_ref[:, tile] = result.astype(out_ref.dtype)

        stage = 0
        for t in range(chunk):
            use = accs[2 * (t % 4) : 2 * (t % 4) + 2]
            code, weight = joined(both_ref, base + t), joined(both_ref, base + t, 2)
            stage = bounce_passes(code, weight, lhs_ref, slot_ref, first, pairs, use, stage)
            if t:
                finish(t - 1)
        finish(chunk - 1)

    pl.run_scoped(body, *accumulators(padded(coeffs), 4))


def far_pass(slots, both, total, albedo, source, first, count, shift, added, dtype, shards, chunk):
    tiles, coeffs, _ = total.shape
    rows = both.shape[2]
    tall = padded(coeffs)
    share = tiles // shards
    unpack = isinstance(source, list)
    operands = list(source) if unpack else [source]
    lhs_shape = (count * PER_OWNER, 2, tall, rows // 2)
    extra = [jax.ShapeDtypeStruct(lhs_shape, jnp.bfloat16)] if unpack else []
    flops = 2 * tall * rows * share * TILE * 2 * count
    result = pl.pallas_call(
        functools.partial(
            far_kernel, count, coeffs, first, unpack, added is not None, 4.0 * math.pi / NDIR, shift, chunk
        ),
        grid=(share // chunk,),
        in_specs=[vmem()] * (4 + len(operands) + (added is not None)),
        out_specs=[vmem()] * (1 + len(extra)),
        out_shape=[jax.ShapeDtypeStruct((coeffs, share * TILE), dtype)] + extra,
        scratch_shapes=[pltpu.VMEM((2, coeffs + tall + 8, rows), jnp.float32)] * unpack,
        compiler_params=limits(16),
        cost_estimate=pl.CostEstimate(flops=flops, bytes_accessed=4 << 20, transcendentals=0),
        name=f"far_{shift}",
    )(slots, both, total, albedo, *operands, *([] if added is None else [added]))
    return (result[0], result[1]) if unpack else result[0]


def listed_by_exchange(me, occluder_list, blocks):
    clusters, slots = occluder_list.shape
    held, coeffs, dirs = blocks.shape
    slot_index = lax.iota(jnp.int32, slots)
    owners = occluder_list // held
    here = owners == me
    position = jnp.cumsum(here.astype(jnp.int32), axis=1) - 1
    matched = here[:, None, :] & (position[:, None, :] == lax.iota(jnp.int32, PER_OWNER)[None, :, None])
    chosen = jnp.sum(jnp.where(matched, (occluder_list - me * held)[:, None, :], 0), axis=2)
    outgoing = jnp.take(blocks, chosen, axis=0)
    incoming = lax.all_to_all(outgoing, "cluster", split_axis=0, concat_axis=0, tiled=True)
    own = owners[me]
    earlier = (own[None, :] == own[:, None]) & (slot_index[None, :] < slot_index[:, None])
    row = own * PER_OWNER + jnp.sum(earlier.astype(jnp.int32), axis=1)
    entries = jnp.take(incoming.reshape(clusters * PER_OWNER, coeffs, dirs), row, axis=0)
    pairs = entries.reshape(slots // PER_OWNER, PER_OWNER * coeffs, dirs)
    return slot_index, [pairs[i] for i in range(slots // PER_OWNER)]


def per_device(n_cluster, n_dir, ray_code, occluder_list, list_count, normal_azimuth, normal_height, albedo, radiance):
    rows, verts = ray_code.shape

    axis_x, axis_y, axis_z = sphere_points(NDIR)
    table = harmonic_table(axis_x, axis_y, axis_z, SHORD).astype(np.float32)
    table = np.pad(table, ((0, padded(table.shape[0]) - table.shape[0]), (0, 0)))
    high = table.astype(jnp.bfloat16)
    low = (table - high.astype(np.float32)).astype(jnp.bfloat16)
    dirs = np.stack([axis_x, axis_y, axis_z] + [np.zeros_like(axis_x)] * 125, axis=1)

    lines = [a.reshape(verts // 128, 128) for a in (normal_azimuth, normal_height, albedo)]
    sources = (*lines, jnp.asarray(dirs), jnp.asarray(high), jnp.asarray(low))
    if n_cluster <= 8 and n_cluster & (n_cluster - 1) == 0:
        blocks = jnp.transpose(radiance, (1, 0, 2))
        slots, live, tables, outgoing = outgoing_pairs(occluder_list, list_count, blocks, sources)
        pairs = list(outgoing)
        for k in range(1, n_cluster):
            pairs[k] = lax.ppermute(outgoing[k], "cluster", [(i, i ^ k) for i in range(n_cluster)])
    else:
        me = lax.axis_index("cluster").astype(jnp.int32)
        index, pairs = listed_by_exchange(me, occluder_list, radiance)
        slots = jnp.broadcast_to(index.astype(jnp.bfloat16)[:, None, None], index.shape + (16, 128))
        live = jnp.broadcast_to(list_count[me].astype(jnp.bfloat16), (16, 128))
        tables = loaded_tables(sources, rows)
    split = len(pairs) // 2

    chunk = math.gcd(8, verts // n_dir // TILE)
    total, both = near_pass(slots, live, ray_code, tables, pairs[:split], 0, math.gcd(4, chunk))
    albedo = tables[2]

    def far(source, shift, added, dtype):
        return far_pass(
            slots, both, total, albedo, source, PER_OWNER * split, len(pairs) - split, shift, added, dtype,
            n_dir, chunk,
        )

    def swap(value, mask):
        return lax.ppermute(value, "dir", [(i, i ^ mask) for i in range(n_dir)])

    if n_dir == 4:
        part_3, lhs = far(pairs[split:], 3, None, jnp.bfloat16)
        part_2 = far(lhs, 2, swap(part_3, 1), jnp.bfloat16)
        part_2 = swap(part_2, 2)
        part_1 = swap(far(lhs, 1, None, jnp.bfloat16), 1)
        kept = far(lhs, 0, part_1, jnp.float32)
        return (kept + part_2.astype(jnp.float32)).astype(jnp.bfloat16)
    kept, lhs = far(pairs[split:], 0, None, jnp.float32)
    for mask in range(1, n_dir):
        kept = kept + swap(far(lhs, mask, None, jnp.bfloat16), mask).astype(jnp.float32)
    return kept.astype(jnp.bfloat16)


def solution(mesh):
    return jax.shard_map(
        functools.partial(per_device, mesh.shape["cluster"], mesh.shape["dir"]),
        mesh=mesh,
        in_specs=(P("dir", "cluster"), P(), P(), P("cluster"), P("cluster"), P("cluster"), P("cluster", None, "dir")),
        out_specs=P(None, ("cluster", "dir")),
        check_vma=False,
    )
```
